32 devices in a mesh: branch: 4 (over z), row: 4 (over y, x), col: 2 (over core).
Axes of the slice: x: 2, y: 2, z: 4, core: 2. Of those that a mesh axis runs over, the one named last changes fastest.
Arguments:
- section_in: bfloat16 [4, 4, 2, 48, 4096], P('branch', 'row', 'col'), may hold values from -6 to 6
- conv_weight: bfloat16 [4, 2, 3, 3, 384, 384], P('branch'), may hold values from -1 to 1, as said below
- conv_bias: float32 [4, 2, 384], P('branch'), may hold values from -3 to 3
- join_weight: bfloat16 [720, 720], replicated, may hold values from -0.4375 to 0.4375
- join_bias: float32 [720], replicated, may hold values from -3 to 3
Outputs:
- joined_first: bfloat16 [48, 128, 256], P(None, ('branch', 'row'), 'col')
- joined_second: bfloat16 [96, 64, 128], P(None, ('branch', 'row'), 'col')
- joined_third: bfloat16 [192, 32, 64], P(None, ('branch', 'row'), 'col')
- joined_fourth: bfloat16 [384, 16, 32], P(None, ('branch', 'row'), 'col')
The draws below stay inside these ranges and needn't reach their ends.
Inputs may be any that keep to these rules, and one draw needn't show every extreme that they name: `conv_weight`: entries of branch b's kernels have standard deviation (9 * 2^b * 48) ** -0.5; entries outside the C_b x C_b corner are drawn too and unused.
All inputs are finite; a program needn't handle non-finite values.
Results may differ from the reference program's by a relative error of at most 0.0075.
Values may be sent and summed in bfloat16 or wider, within the bound.
A program may use at most 128 MiB of HBM per device.

```python
import jax
import jax.numpy as jnp
from jax import lax

WIDTH = 48
TH = 32
TW = 128
N_BRANCH = 4
N_ROW = 4
N_COL = 2


def draw_conv_weight(key, part):
    array_dims = (4, 2, 3, 3, 8 * WIDTH, 8 * WIDTH)
    fan_scale = (9.0 * WIDTH * 2.0 ** jnp.arange(4, dtype=jnp.float32)) ** (-0.5)
    values = jax.random.normal(key, array_dims, jnp.float32)
    values = jnp.clip(values, -6.0, 6.0)
    return (values * fan_scale[:, None, None, None, None, None]).astype(jnp.bfloat16)


def block_scale(rng, shape, pieces, low, largest):
    gain = 1.0
    for position, parts in pieces:
        draws = jax.random.uniform(jax.random.fold_in(jax.random.fold_in(rng, 6), position), (parts,), jnp.float32, low / len(pieces), largest / len(pieces))
        gain = gain * jnp.repeat(jnp.exp(draws), shape[position] // parts).reshape((-1,) + (1,) * (len(shape) - 1 - position))
    return gain


def bell_draw(stream_key, dims, width, limit, split=(), held_as=jnp.bfloat16):
    values = width * jax.random.normal(stream_key, dims, jnp.float32)
    if split:
        values = values * block_scale(stream_key, dims, split, -0.22, 0.18)
    return jnp.clip(values, -limit, limit).astype(held_as)


def setup_inputs(seed: int = 0) -> dict:
    key_list = jax.random.split(jax.random.key(seed), 6)
    section_in = bell_draw(key_list[0], (N_BRANCH, N_ROW, N_COL, WIDTH, TH * TW), 1.0, 6.0, ((0, 4), (1, 4), (2, 2)))
    conv_weight = draw_conv_weight(jax.random.fold_in(key_list[5], 71), 0)
    conv_bias = bell_draw(key_list[2], (N_BRANCH, 2, 8 * WIDTH), 0.5, 3.0, ((0, 4),), jnp.float32)
    join_weight = bell_draw(key_list[3], (15 * WIDTH, 15 * WIDTH), (4 * WIDTH) ** -0.5, 0.4375)
    join_bias = bell_draw(key_list[4], (15 * WIDTH,), 0.5, 3.0, (), jnp.float32)
    return {"section_in": section_in, "conv_weight": conv_weight, "conv_bias": conv_bias, "join_weight": join_weight, "join_bias": join_bias}


def branch_map(section_in, branch_level):
    channels = WIDTH * 2 ** branch_level
    tile_rows = TH // 2 ** branch_level
    tile_cols = TW // 2 ** branch_level
    packed = section_in[branch_level][:, :, :, : (TH * TW) // 2 ** branch_level]
    packed = packed.reshape(N_ROW, N_COL, channels, tile_rows, tile_cols)
    return packed.transpose(2, 0, 3, 1, 4).reshape(channels, N_ROW * tile_rows, N_COL * tile_cols)


def conv_same(field, kernel):
    result = lax.conv_general_dilated(
        field[None].astype(jnp.float32),
        kernel.astype(jnp.float32).transpose(2, 3, 0, 1),
        (1, 1),
        "SAME",
        dimension_numbers=("NCHW", "OIHW", "NCHW"),
        precision=lax.Precision.HIGHEST,
    )
    return result[0]


def pooled(tile_data, factor):
    channels, height, breadth = tile_data.shape
    blocks = tile_data.astype(jnp.float32).reshape(channels, height // factor, factor, breadth // factor, factor)
    return jnp.mean(blocks, axis=(2, 4)).astype(jnp.bfloat16)


def upsample(tile_data, factor):
    channels, height, breadth = tile_data.shape
    spread = jnp.broadcast_to(tile_data[:, :, None, :, None], (channels, height, factor, breadth, factor))
    return spread.reshape(channels, height * factor, breadth * factor)


def mix_block(join_weight, target, source, tile_data):
    target_start = (2 ** target - 1) * WIDTH
    source_start = (2 ** source - 1) * WIDTH
    target_width = WIDTH * 2 ** target
    source_width = WIDTH * 2 ** source
    block = join_weight[target_start:target_start + target_width, source_start:source_start + source_width]
    channels, height, breadth = tile_data.shape
    product = jnp.dot(block, tile_data.reshape(channels, height * breadth), preferred_element_type=jnp.float32)
    return product.astype(jnp.bfloat16).reshape(target_width, height, breadth)


def reference(section_in, conv_weight, conv_bias, join_weight, join_bias):
    settled = []
    for branch_level in range(4):
        channels = WIDTH * 2 ** branch_level
        inputs = branch_map(section_in, branch_level)
        kernel_first = conv_weight[branch_level, 0, :, :, :channels, :channels]
        kernel_second = conv_weight[branch_level, 1, :, :, :channels, :channels]
        hidden = jax.nn.relu(conv_same(inputs, kernel_first) + conv_bias[branch_level, 0, :channels, None, None])
        hidden = hidden.astype(jnp.bfloat16)
        after = conv_same(hidden, kernel_second) + conv_bias[branch_level, 1, :channels, None, None]
        settled.append(jax.nn.relu(after + inputs.astype(jnp.float32)).astype(jnp.bfloat16))
    outputs = []
    for target in range(4):
        target_start = (2 ** target - 1) * WIDTH
        target_width = WIDTH * 2 ** target
        total_sum = settled[target].astype(jnp.float32) + join_bias[target_start:target_start + target_width, None, None]
        for source in range(4):
            if source < target:
                term = mix_block(join_weight, target, source, pooled(settled[source], 2 ** (target - source)))
                total_sum = total_sum + term.astype(jnp.float32)
            elif source > target:
                term = mix_block(join_weight, target, source, settled[source])
                total_sum = total_sum + upsample(term, 2 ** (source - target)).astype(jnp.float32)
        outputs.append(jax.nn.relu(total_sum).astype(jnp.bfloat16))
    return (outputs[0], outputs[1], outputs[2], outputs[3])
```

```python
from functools import partial

import jax
import jax.numpy as jnp
from jax import lax
from jax.experimental import pallas as pl
from jax.experimental.pallas import tpu as pltpu
from jax.sharding import PartitionSpec as P

WIDTH = 48
TH = 32
TW = 128


def for_sending(shard):

    def short(part):
        return part.astype(jnp.bfloat16) if part.dtype == jnp.float32 else part

    return jax.tree.map(short, shard)


def shifted(shard, axis, by):
    size = lax.axis_size(axis)
    pairs = [(i, i + by) for i in range(size) if 0 <= i + by < size]
    return lax.ppermute(shard, axis, pairs)


def tile_view(container, branch_level):
    pixels = TH * TW >> branch_level
    return container[:, :pixels].reshape(
        WIDTH << branch_level, TH >> branch_level, TW >> branch_level
    )


def tile_pack(tile_data, branch_level):
    flat = tile_data.reshape(WIDTH, TH * TW >> branch_level)
    return jnp.pad(flat, ((0, 0), (0, TH * TW - flat.shape[1])))


def side_length(rim_width):
    return WIDTH * TH * rim_width + 16 * WIDTH * rim_width * rim_width


def row_rims(branch_level, rim_width, container):
    tile_data = tile_view(container, branch_level)
    top_rows = tile_data[:, :rim_width, :].reshape(WIDTH * rim_width, TW)
    bottom_rows = tile_data[:, -rim_width:, :].reshape(WIDTH * rim_width, TW)
    return (top_rows, bottom_rows)


def side_rims(branch_level, rim_width, container, from_above, from_below):
    tile_data = tile_view(container, branch_level)
    channels, tile_rows, tile_cols = tile_data.shape
    upper = from_above.reshape(channels, rim_width, tile_cols)
    lower = from_below.reshape(channels, rim_width, tile_cols)
    west_side = jnp.concatenate(
        [upper[:, :, :rim_width], tile_data[:, :, :rim_width], lower[:, :, :rim_width]], axis=1
    )
    east_side = jnp.concatenate(
        [upper[:, :, -rim_width:], tile_data[:, :, -rim_width:], lower[:, :, -rim_width:]], axis=1
    )
    west_flat = west_side.reshape(-1)
    east_flat = east_side.reshape(-1)
    padding = side_length(rim_width) - west_flat.shape[0]
    return (jnp.pad(west_flat, (0, padding)), jnp.pad(east_flat, (0, padding)))


def halo_round(container, rim_width, level_index):
    top_rows, bottom_rows = lax.switch(
        level_index,
        [partial(row_rims, branch_level, rim_width) for branch_level in range(4)],
        container,
    )
    from_above = jax.tree.map(
        lambda part, own: part.astype(own.dtype),
        shifted(for_sending(bottom_rows), "row", 1),
        bottom_rows,
    )
    from_below = jax.tree.map(
        lambda part, own: part.astype(own.dtype),
        shifted(for_sending(top_rows), "row", -1),
        top_rows,
    )
    west_side, east_side = lax.switch(
        level_index,
        [partial(side_rims, branch_level, rim_width) for branch_level in range(4)],
        container,
        from_above,
        from_below,
    )
    from_left = jax.tree.map(
        lambda part, own: part.astype(own.dtype),
        shifted(for_sending(east_side), "col", 1),
        east_side,
    )
    from_right = jax.tree.map(
        lambda part, own: part.astype(own.dtype),
        shifted(for_sending(west_side), "col", -1),
        west_side,
    )
    return (from_above, from_below, from_left, from_right)


def extended_tile(branch_level, rim_width, container, halo_parts):
    from_above, from_below, from_left, from_right = halo_parts
    tile_data = tile_view(container, branch_level)
    channels, tile_rows, tile_cols = tile_data.shape
    upper = from_above.reshape(channels, rim_width, tile_cols)
    lower = from_below.reshape(channels, rim_width, tile_cols)
    tall = jnp.concatenate([upper, tile_data, lower], axis=1)
    count = channels * (tile_rows + 2 * rim_width) * rim_width
    west_side = from_left[:count].reshape(channels, tile_rows + 2 * rim_width, rim_width)
    east_side = from_right[:count].reshape(channels, tile_rows + 2 * rim_width, rim_width)
    return jnp.concatenate([west_side, tall, east_side], axis=2)


def conv_valid(extended, kernel, offset_bias):
    channels, ext_rows, ext_cols = extended.shape
    out_rows = ext_rows - 2
    out_cols = ext_cols - 2
    total_sum = jnp.zeros((kernel.shape[2], out_rows * out_cols), jnp.float32)
    for row_tap in range(3):
        stacked = jnp.concatenate(
            [
                extended[:, row_tap : row_tap + out_rows, col_tap : col_tap + out_cols]
                for col_tap in range(3)
            ],
            axis=0,
        )
        stacked = stacked.reshape(3 * channels, out_rows * out_cols)
        matrix = jnp.concatenate([kernel[row_tap, col_tap] for col_tap in range(3)], axis=1)
        total_sum = total_sum + jnp.dot(matrix, stacked, preferred_element_type=jnp.float32)
    return total_sum.reshape(-1, out_rows, out_cols) + offset_bias[:, None, None]


def deep_block(
    branch_level, container, halo_parts, kernels, biases, row_place, col_place, row_count, col_count
):
    channels = WIDTH << branch_level
    tile_rows = TH >> branch_level
    tile_cols = TW >> branch_level
    extended = extended_tile(branch_level, 2, container, halo_parts)
    hidden = jax.nn.relu(
        conv_valid(extended, kernels[0, :, :, :channels, :channels], biases[0, :channels])
    )
    row_ids = jnp.arange(tile_rows + 2)
    col_ids = jnp.arange(tile_cols + 2)
    row_outside = (row_ids == 0) & (row_place == 0) | (row_ids == tile_rows + 1) & (
        row_place == row_count - 1
    )
    col_outside = (col_ids == 0) & (col_place == 0) | (col_ids == tile_cols + 1) & (
        col_place == col_count - 1
    )
    inside_mask = jnp.logical_not(row_outside[:, None] | col_outside[None, :])
    hidden = jnp.where(inside_mask[None], hidden, 0.0).astype(jnp.bfloat16)
    inputs = tile_view(container, branch_level)
    after = conv_valid(hidden, kernels[1, :, :, :channels, :channels], biases[1, :channels])
    settled = jax.nn.relu(after + inputs.astype(jnp.float32)).astype(jnp.bfloat16)
    return strip_pack(settled.reshape(channels, tile_rows * tile_cols))


LANES = 128
STRIPS = 4
PIECE_ROWS = WIDTH * TH * TW // (STRIPS * LANES)
MESH = pl.DeviceIdType.MESH


def piece_rows(branch_level):
    pixels = TH * TW // STRIPS >> 2 * branch_level
    return (WIDTH << branch_level) * max(1, pixels // LANES)


def strip_pack(settled):
    pixels = settled.shape[1] // STRIPS
    strips = []
    for strip in range(STRIPS):
        part = settled[:, strip * pixels : (strip + 1) * pixels]
        if pixels >= LANES:
            part = jnp.concatenate(
                [part[:, at : at + LANES] for at in range(0, pixels, LANES)], axis=0
            )
        strips.append(
            jnp.pad(part, ((0, PIECE_ROWS - part.shape[0]), (0, LANES - part.shape[1])))
        )
    return jnp.stack(strips)


def block_mask(fine_level, coarse_level):
    fine_cols = TW >> fine_level
    coarse_cols = TW >> coarse_level
    fine = TH * TW // STRIPS >> 2 * fine_level
    coarse = TH * TW // STRIPS >> 2 * coarse_level
    shift = coarse_level - fine_level
    pixel = lax.broadcasted_iota(jnp.int32, (fine, 1), 0)
    row = lax.shift_right_logical(pixel, fine_cols.bit_length() - 1 + shift)
    col = lax.shift_right_logical(pixel & (fine_cols - 1), shift)
    home = row * coarse_cols + col
    target = lax.broadcasted_iota(jnp.int32, (fine, coarse), 1)
    return jnp.where(home == target, 1.0, 0.0).astype(jnp.bfloat16)


def mixed(weight_ref, target, source, tile_data):
    start = ((1 << source) - 1) * WIDTH
    low = start // LANES * LANES
    high = min(-(-(start + tile_data.shape[0]) // LANES) * LANES, weight_ref.shape[1])
    pieces = []
    if start > low:
        pieces.append(jnp.zeros((start - low, tile_data.shape[1]), tile_data.dtype))
    pieces.append(tile_data)
    if high > start + tile_data.shape[0]:
        pieces.append(
            jnp.zeros((high - start - tile_data.shape[0], tile_data.shape[1]), tile_data.dtype)
        )
    rows = ((1 << target) - 1) * WIDTH
    return jnp.dot(
        weight_ref[rows : rows + (WIDTH << target), low:high],
        jnp.concatenate(pieces, axis=0),
        preferred_element_type=jnp.float32,
    ).astype(jnp.bfloat16)


def join_strip(maps, masks, weight_ref, bias_ref, out_refs):
    for target in range(4):
        start = ((1 << target) - 1) * WIDTH
        total = maps[target].astype(jnp.float32) + bias_ref[start : start + (WIDTH << target), :]
        for source in range(4):
            if source < target:
                share = 0.25 ** (target - source)
                shrunk = jnp.dot(
                    maps[source], masks[source, target], preferred_element_type=jnp.float32
                )
                term = mixed(weight_ref, target, source, (shrunk * share).astype(jnp.bfloat16))
                total = total + term.astype(jnp.float32)
            elif source > target:
                term = mixed(weight_ref, target, source, maps[source])
                total = total + lax.dot_general(
                    term,
                    masks[target, source],
                    (((1,), (1,)), ((), ())),
                    preferred_element_type=jnp.float32,
                )
        out_refs[target][...] = jnp.maximum(total, 0.0).astype(jnp.bfloat16)


def exchange_join(
    strips_ref, weight_ref, bias_ref, out0, out1, out2, out3, held, send_sem, recv_sem, own_sem
):
    level = lax.axis_index("branch")
    place = lax.axis_index("row")
    col = lax.axis_index("col")
    home = level == place

    barrier = pltpu.get_barrier_semaphore()
    for other in range(4):

        @pl.when(jnp.logical_not(home & (level == other)))
        def _():
            pl.semaphore_signal(
                barrier, inc=1, device_id=(other, level, col), device_id_type=MESH
            )

    pl.semaphore_wait(barrier, jnp.where(home, 3, 4))

    def remote(source, strip):
        rows = piece_rows(source)
        return pltpu.make_async_remote_copy(
            src_ref=strips_ref.at[strip, 0:rows],
            dst_ref=held.at[source, 0:rows],
            send_sem=send_sem.at[strip],
            recv_sem=recv_sem.at[source],
            device_id=(place, strip, col),
            device_id_type=MESH,
        )

    def own(source):
        rows = piece_rows(source)
        return pltpu.make_async_copy(
            strips_ref.at[source, 0:rows], held.at[source, 0:rows], own_sem
        )

    for source in range(4):
        for step in range(4):
            strip = (source + 1 + step) % 4

            @pl.when((level == source) & jnp.logical_not(home & (level == strip)))
            def _():
                remote(source, strip).start()

        @pl.when((level == source) & home)
        def _():
            own(source).start()

    masks = {
        (fine, coarse): block_mask(fine, coarse)
        for fine in range(3)
        for coarse in range(fine + 1, 4)
    }

    for source in range(4):

        @pl.when(jnp.logical_not(home & (level == source)))
        def _():
            remote(source, 0).wait_recv()

        @pl.when((level == source) & home)
        def _():
            own(source).wait()

    maps = []
    for source in range(4):
        channels = WIDTH << source
        pixels = TH * TW // STRIPS >> 2 * source
        if pixels >= LANES:
            maps.append(
                jnp.concatenate(
                    [
                        held[source, at * channels : (at + 1) * channels]
                        for at in range(pixels // LANES)
                    ],
                    axis=1,
                )
            )
        else:
            maps.append(held[source, 0:channels][:, :pixels])
    join_strip(maps, masks, weight_ref, bias_ref, (out0, out1, out2, out3))

    for source in range(4):
        for strip in range(4):

            @pl.when((level == source) & jnp.logical_not(home & (level == strip)))
            def _():
                remote(source, strip).wait_send()


def joined(strips, join_weight, join_bias):
    vmem = pl.BlockSpec(memory_space=pltpu.VMEM)
    return pl.pallas_call(
        exchange_join,
        out_shape=[
            jax.ShapeDtypeStruct(
                (WIDTH << b, TH * TW // STRIPS >> 2 * b), jnp.bfloat16
            )
            for b in range(4)
        ],
        in_specs=[vmem] * 3,
        out_specs=[vmem] * 4,
        scratch_shapes=[
            pltpu.VMEM((4, PIECE_ROWS, LANES), jnp.bfloat16),
            pltpu.SemaphoreType.DMA((4,)),
            pltpu.SemaphoreType.DMA((4,)),
            pltpu.SemaphoreType.DMA,
        ],
        compiler_params=pltpu.CompilerParams(collective_id=0, has_side_effects=True),
        name="exchange_join",
    )(strips, join_weight, join_bias[:, None])


def local(section_in, conv_weight, conv_bias, join_weight, join_bias):
    level_index = lax.axis_index("branch")
    row_place = lax.axis_index("row")
    col_place = lax.axis_index("col")
    row_count = lax.axis_size("row")
    col_count = lax.axis_size("col")
    container = section_in[0, 0, 0]
    kernels = conv_weight[0]
    biases = conv_bias[0]
    halo_parts = halo_round(container, 2, level_index)
    strips = lax.switch(
        level_index,
        [
            partial(deep_block, branch_level, row_count=row_count, col_count=col_count)
            for branch_level in range(4)
        ],
        container,
        halo_parts,
        kernels,
        biases,
        row_place,
        col_place,
    )
    outs = joined(strips, join_weight, join_bias)
    return tuple(
        out.reshape(WIDTH << b, (TH >> b) // STRIPS, TW >> b) for b, out in enumerate(outs)
    )


def solution(mesh):
    in_specs = (
        P("branch", "row", "col", None, None),
        P("branch", None, None, None, None, None),
        P("branch", None, None),
        P(),
        P(),
    )
    out_specs = (
        P(None, ("branch", "row"), "col"),
        P(None, ("branch", "row"), "col"),
        P(None, ("branch", "row"), "col"),
        P(None, ("branch", "row"), "col"),
    )
    return jax.shard_map(local, mesh=mesh, in_specs=in_specs, out_specs=out_specs, check_vma=False)
```

```python
from functools import partial

import jax
import jax.numpy as jnp
from jax import lax
from jax.experimental import pallas as pl
from jax.experimental.pallas import tpu as pltpu
from jax.sharding import PartitionSpec as P

WIDTH = 48
TH = 32
TW = 128


def for_sending(shard):

    def short(part):
        return part.astype(jnp.bfloat16) if part.dtype == jnp.float32 else part

    return jax.tree.map(short, shard)


def shifted(shard, axis, by):
    size = lax.axis_size(axis)
    pairs = [(i, i + by) for i in range(size) if 0 <= i + by < size]
    return lax.ppermute(shard, axis, pairs)


def tile_view(container, branch_level):
    pixels = TH * TW >> branch_level
    return container[:, :pixels].reshape(
        WIDTH << branch_level, TH >> branch_level, TW >> branch_level
    )


def tile_pack(tile_data, branch_level):
    flat = tile_data.reshape(WIDTH, TH * TW >> branch_level)
    return jnp.pad(flat, ((0, 0), (0, TH * TW - flat.shape[1])))


def side_length(rim_width):
    return WIDTH * TH * rim_width + 16 * WIDTH * rim_width * rim_width


def row_rims(branch_level, rim_width, container):
    tile_data = tile_view(container, branch_level)
    top_rows = tile_data[:, :rim_width, :].reshape(WIDTH * rim_width, TW)
    bottom_rows = tile_data[:, -rim_width:, :].reshape(WIDTH * rim_width, TW)
    return (top_rows, bottom_rows)


def side_rims(branch_level, rim_width, container, from_above, from_below):
    tile_data = tile_view(container, branch_level)
    channels, tile_rows, tile_cols = tile_data.shape
    upper = from_above.reshape(channels, rim_width, tile_cols)
    lower = from_below.reshape(channels, rim_width, tile_cols)
    west_side = jnp.concatenate(
        [upper[:, :, :rim_width], tile_data[:, :, :rim_width], lower[:, :, :rim_width]], axis=1
    )
    east_side = jnp.concatenate(
        [upper[:, :, -rim_width:], tile_data[:, :, -rim_width:], lower[:, :, -rim_width:]], axis=1
    )
    west_flat = west_side.reshape(-1)
    east_flat = east_side.reshape(-1)
    padding = side_length(rim_width) - west_flat.shape[0]
    return (jnp.pad(west_flat, (0, padding)), jnp.pad(east_flat, (0, padding)))


def halo_round(container, rim_width, level_index):
    top_rows, bottom_rows = lax.switch(
        level_index,
        [partial(row_rims, branch_level, rim_width) for branch_level in range(4)],
        container,
    )
    from_above = jax.tree.map(
        lambda part, own: part.astype(own.dtype),
        shifted(for_sending(bottom_rows), "row", 1),
        bottom_rows,
    )
    from_below = jax.tree.map(
        lambda part, own: part.astype(own.dtype),
        shifted(for_sending(top_rows), "row", -1),
        top_rows,
    )
    west_side, east_side = lax.switch(
        level_index,
        [partial(side_rims, branch_level, rim_width) for branch_level in range(4)],
        container,
        from_above,
        from_below,
    )
    from_left = jax.tree.map(
        lambda part, own: part.astype(own.dtype),
        shifted(for_sending(east_side), "col", 1),
        east_side,
    )
    from_right = jax.tree.map(
        lambda part, own: part.astype(own.dtype),
        shifted(for_sending(west_side), "col", -1),
        west_side,
    )
    return (from_above, from_below, from_left, from_right)


def row_pitch(branch_level):
    return 2 * TW >> branch_level


def extended_flat(branch_level, container, halo_parts):
    from_above, from_below, from_left, from_right = halo_parts
    tile_data = tile_view(container, branch_level)
    channels, tile_rows, tile_cols = tile_data.shape
    upper = from_above.reshape(channels, 2, tile_cols)
    lower = from_below.reshape(channels, 2, tile_cols)
    tall = jnp.concatenate([upper, tile_data, lower], axis=1)
    ext_rows = tile_rows + 4
    count = channels * ext_rows * 2
    west_side = from_left[:count].reshape(channels, ext_rows, 2)
    east_side = from_right[:count].reshape(channels, ext_rows, 2)
    west_next = jnp.concatenate([west_side[:, 1:], west_side[:, :1]], axis=1)
    gap = jnp.zeros(
        (channels, ext_rows, row_pitch(branch_level) - tile_cols - 4), tile_data.dtype
    )
    return jnp.concatenate([tall, east_side, gap, west_next], axis=2).reshape(channels, -1)


def tap_stack(field, pitch, rows_kept):
    total = field.shape[1]
    views = {}
    for dx in (-1, 0, 1):
        if pitch % LANES == 0:
            view = field if dx == 0 else pltpu.roll(field, -dx % total, 1)
            view = view.astype(jnp.bfloat16)
            if rows_kept:
                step = LANES
                view = jnp.concatenate(
                    [view[:, y * pitch : y * pitch + LANES] for y in range(1, rows_kept + 3)],
                    axis=1,
                )
                size = rows_kept * LANES
            else:
                step = pitch
                view = jnp.concatenate([view[:, total - pitch :], view, view[:, :pitch]], axis=1)
                size = total
            for dy in range(3):
                views[dy, dx] = view[:, dy * step : dy * step + size]
        else:
            for dy in range(3):
                shift = -(dx + (dy - 1) * pitch) % total
                view = field if shift == 0 else pltpu.roll(field, shift, 1)
                views[dy, dx] = view.astype(jnp.bfloat16)
    return jnp.concatenate([views[dy, dx] for dy in range(3) for dx in (-1, 0, 1)], axis=0)


def block_kernel(branch_level, ext_ref, first_ref, second_ref, bias_ref, strips_ref):
    pitch = row_pitch(branch_level)
    tile_rows, tile_cols = TH >> branch_level, TW >> branch_level
    channels, total = ext_ref.shape
    place, col = lax.axis_index("row"), lax.axis_index("col")
    field = ext_ref[...].astype(jnp.float32)
    hidden = jnp.dot(
        first_ref[...], tap_stack(field, pitch, 0), preferred_element_type=jnp.float32
    )
    hidden = jnp.maximum(hidden + bias_ref[0], 0.0)
    pixel = lax.broadcasted_iota(jnp.int32, (1, total), 1) + 1
    y = lax.shift_right_logical(pixel, pitch.bit_length() - 1)
    x = pixel & (pitch - 1)
    top = jnp.where(place == 0, 1, -1)
    bottom = jnp.where(place == lax.axis_size("row") - 1, tile_rows + 2, -1)
    left = jnp.where(col == 0, 0, -1)
    right = jnp.where(col == lax.axis_size("col") - 1, tile_cols + 1, -1)
    inside = (y != top) & (y != bottom) & (x != left) & (x != right)
    hidden = jnp.where(inside, hidden, 0.0).astype(jnp.bfloat16).astype(jnp.float32)
    narrow = tile_cols == LANES
    rows_kept = tile_rows if narrow else 0
    after = jnp.dot(
        second_ref[...], tap_stack(hidden, pitch, rows_kept), preferred_element_type=jnp.float32
    )
    if narrow:
        field = jnp.concatenate(
            [field[:, y * pitch : y * pitch + LANES] for y in range(2, tile_rows + 2)], axis=1
        )
    settled = jnp.maximum(after + bias_ref[1] + field, 0.0)
    strip_rows = tile_rows // STRIPS
    lane = lax.broadcasted_iota(jnp.int32, (1, LANES), 1)
    for strip in range(STRIPS):
        groups = []
        if narrow:
            groups = [
                settled[:, y * LANES : (y + 1) * LANES]
                for y in range(strip * strip_rows, (strip + 1) * strip_rows)
            ]
        else:
            per_group = min(LANES // tile_cols, strip_rows)
            for start in range(0, strip_rows, per_group):
                merged = None
                for turn in range(per_group):
                    at = (strip * strip_rows + start + turn + 2) * pitch
                    part = settled[:, at // LANES * LANES : at // LANES * LANES + LANES]
                    shift = (turn * tile_cols - at) % LANES
                    part = pltpu.roll(part, shift, 1) if shift else part
                    merged = part if turn == 0 else jnp.where(lane < turn * tile_cols, merged, part)
                groups.append(merged)
        for at, group in enumerate(groups):
            strips_ref[strip, at * channels : (at + 1) * channels] = group.astype(jnp.bfloat16)


def deep_block(branch_level, container, halo_parts, kernels, biases):
    channels = WIDTH << branch_level
    extended = extended_flat(branch_level, container, halo_parts)
    first, second = (
        jnp.concatenate(
            [
                kernels[layer, dy, dx, :channels, :channels]
                for dy in range(3)
                for dx in range(3)
            ],
            axis=1,
        )
        for layer in range(2)
    )
    vmem = pl.BlockSpec(memory_space=pltpu.VMEM)
    return pl.pallas_call(
        partial(block_kernel, branch_level),
        out_shape=jax.ShapeDtypeStruct((STRIPS, PIECE_ROWS, LANES), jnp.bfloat16),
        in_specs=[vmem] * 4,
        out_specs=vmem,
        compiler_params=pltpu.CompilerParams(vmem_limit_bytes=60 << 20),
        name=f"block_{branch_level}",
    )(extended, first, second, biases[:, :channels, None])


LANES = 128
STRIPS = 4
PIECE_ROWS = WIDTH * TH * TW // (STRIPS * LANES)
MESH = pl.DeviceIdType.MESH


def piece_rows(branch_level):
    pixels = TH * TW // STRIPS >> 2 * branch_level
    return (WIDTH << branch_level) * max(1, pixels // LANES)


def block_mask(fine_level, coarse_level):
    fine_cols = TW >> fine_level
    coarse_cols = TW >> coarse_level
    fine = TH * TW // STRIPS >> 2 * fine_level
    coarse = TH * TW // STRIPS >> 2 * coarse_level
    shift = coarse_level - fine_level
    pixel = lax.broadcasted_iota(jnp.int32, (fine, 1), 0)
    row = lax.shift_right_logical(pixel, fine_cols.bit_length() - 1 + shift)
    col = lax.shift_right_logical(pixel & (fine_cols - 1), shift)
    home = row * coarse_cols + col
    target = lax.broadcasted_iota(jnp.int32, (fine, coarse), 1)
    return jnp.where(home == target, 1.0, 0.0).astype(jnp.bfloat16)


def mixed(weight_ref, target, source, tile_data):
    start = ((1 << source) - 1) * WIDTH
    low = start // LANES * LANES
    high = min(-(-(start + tile_data.shape[0]) // LANES) * LANES, weight_ref.shape[1])
    pieces = []
    if start > low:
        pieces.append(jnp.zeros((start - low, tile_data.shape[1]), tile_data.dtype))
    pieces.append(tile_data)
    if high > start + tile_data.shape[0]:
        pieces.append(
            jnp.zeros((high - start - tile_data.shape[0], tile_data.shape[1]), tile_data.dtype)
        )
    rows = ((1 << target) - 1) * WIDTH
    return jnp.dot(
        weight_ref[rows : rows + (WIDTH << target), low:high],
        jnp.concatenate(pieces, axis=0),
        preferred_element_type=jnp.float32,
    ).astype(jnp.bfloat16)


def join_strip(maps, masks, weight_ref, bias_ref, out_refs):
    for target in range(4):
        start = ((1 << target) - 1) * WIDTH
        total = maps[target].astype(jnp.float32) + bias_ref[start : start + (WIDTH << target), :]
        for source in range(4):
            if source < target:
                share = 0.25 ** (target - source)
                shrunk = jnp.dot(
                    maps[source], masks[source, target], preferred_element_type=jnp.float32
                )
                term = mixed(weight_ref, target, source, (shrunk * share).astype(jnp.bfloat16))
                total = total + term.astype(jnp.float32)
            elif source > target:
                term = mixed(weight_ref, target, source, maps[source])
                total = total + lax.dot_general(
                    term,
                    masks[target, source],
                    (((1,), (1,)), ((), ())),
                    preferred_element_type=jnp.float32,
                )
        out_refs[target][...] = jnp.maximum(total, 0.0).astype(jnp.bfloat16)


def exchange_join(
    strips_ref, weight_ref, bias_ref, out0, out1, out2, out3, held, send_sem, recv_sem, own_sem
):
    level = lax.axis_index("branch")
    place = lax.axis_index("row")
    col = lax.axis_index("col")
    home = level == place

    barrier = pltpu.get_barrier_semaphore()
    for other in range(4):

        @pl.when(jnp.logical_not(home & (level == other)))
        def _():
            pl.semaphore_signal(
                barrier, inc=1, device_id=(other, level, col), device_id_type=MESH
            )

    pl.semaphore_wait(barrier, jnp.where(home, 3, 4))

    def remote(source, strip):
        rows = piece_rows(source)
        return pltpu.make_async_remote_copy(
            src_ref=strips_ref.at[strip, 0:rows],
            dst_ref=held.at[source, 0:rows],
            send_sem=send_sem.at[strip],
            recv_sem=recv_sem.at[source],
            device_id=(place, strip, col),
            device_id_type=MESH,
        )

    def own(source):
        rows = piece_rows(source)
        return pltpu.make_async_copy(
            strips_ref.at[source, 0:rows], held.at[source, 0:rows], own_sem
        )

    for source in range(4):
        for step in range(4):
            strip = (source + 1 + step) % 4

            @pl.when((level == source) & jnp.logical_not(home & (level == strip)))
            def _():
                remote(source, strip).start()

        @pl.when((level == source) & home)
        def _():
            own(source).start()

    masks = {
        (fine, coarse): block_mask(fine, coarse)
        for fine in range(3)
        for coarse in range(fine + 1, 4)
    }

    for source in range(4):

        @pl.when(jnp.logical_not(home & (level == source)))
        def _():
            remote(source, 0).wait_recv()

        @pl.when((level == source) & home)
        def _():
            own(source).wait()

    maps = []
    for source in range(4):
        channels = WIDTH << source
        pixels = TH * TW // STRIPS >> 2 * source
        if pixels >= LANES:
            maps.append(
                jnp.concatenate(
                    [
                        held[source, at * channels : (at + 1) * channels]
                        for at in range(pixels // LANES)
                    ],
                    axis=1,
                )
            )
        else:
            maps.append(held[source, 0:channels][:, :pixels])
    join_strip(maps, masks, weight_ref, bias_ref, (out0, out1, out2, out3))

    for source in range(4):
        for strip in range(4):

            @pl.when((level == source) & jnp.logical_not(home & (level == strip)))
            def _():
                remote(source, strip).wait_send()


def joined(strips, join_weight, join_bias):
    vmem = pl.BlockSpec(memory_space=pltpu.VMEM)
    return pl.pallas_call(
        exchange_join,
        out_shape=[
            jax.ShapeDtypeStruct(
                (WIDTH << b, TH * TW // STRIPS >> 2 * b), jnp.bfloat16
            )
            for b in range(4)
        ],
        in_specs=[vmem] * 3,
        out_specs=[vmem] * 4,
        scratch_shapes=[
            pltpu.VMEM((4, PIECE_ROWS, LANES), jnp.bfloat16),
            pltpu.SemaphoreType.DMA((4,)),
            pltpu.SemaphoreType.DMA((4,)),
            pltpu.SemaphoreType.DMA,
        ],
        compiler_params=pltpu.CompilerParams(collective_id=0, has_side_effects=True),
        name="exchange_join",
    )(strips, join_weight, join_bias[:, None])


def local(section_in, conv_weight, conv_bias, join_weight, join_bias):
    level_index = lax.axis_index("branch")
    container = section_in[0, 0, 0]
    kernels = conv_weight[0]
    biases = conv_bias[0]
    halo_parts = halo_round(container, 2, level_index)
    strips = lax.switch(
        level_index,
        [
            partial(deep_block, branch_level) for branch_level in range(4)
        ],
        container,
        halo_parts,
        kernels,
        biases,
    )
    outs = joined(strips, join_weight, join_bias)
    return tuple(
        out.reshape(WIDTH << b, (TH >> b) // STRIPS, TW >> b) for b, out in enumerate(outs)
    )


def solution(mesh):
    in_specs = (
        P("branch", "row", "col", None, None),
        P("branch", None, None, None, None, None),
        P("branch", None, None),
        P(),
        P(),
    )
    out_specs = (
        P(None, ("branch", "row"), "col"),
        P(None, ("branch", "row"), "col"),
        P(None, ("branch", "row"), "col"),
        P(None, ("branch", "row"), "col"),
    )
    return jax.shard_map(local, mesh=mesh, in_specs=in_specs, out_specs=out_specs, check_vma=False)
```

```python
from functools import partial

import jax
import jax.numpy as jnp
from jax import lax
from jax.experimental import pallas as pl
from jax.experimental.pallas import tpu as pltpu
from jax.sharding import PartitionSpec as P

WIDTH = 48
TH = 32
TW = 128


def row_pitch(branch_level):
    return 2 * TW >> branch_level


def natural_tile(branch_level, container_ref):
    pixels = TH * TW >> 2 * branch_level
    if branch_level == 0:
        return container_ref[...].astype(jnp.float32)
    channels = WIDTH << branch_level
    parts = []
    for part in range(1 << branch_level):
        at = part * pixels
        low = at // LANES * LANES
        piece = container_ref[:, low : low + max(pixels, LANES)]
        if at > low:
            piece = pltpu.roll(piece.astype(jnp.float32), LANES - at + low, 1).astype(jnp.bfloat16)
        parts.append(piece)
    held = lax.broadcasted_iota(jnp.int32, (1, channels), 1)
    part = sum((held >= WIDTH * turn).astype(jnp.int32) for turn in range(1, 1 << branch_level))
    home = ((held - WIDTH * part) << branch_level) + part
    order = jnp.where(lax.broadcasted_iota(jnp.int32, (channels, channels), 0) == home, 1.0, 0.0)
    return jnp.dot(
        order.astype(jnp.bfloat16),
        jnp.concatenate(parts, axis=0),
        preferred_element_type=jnp.float32,
    )


def turned(group, shift):
    shift = shift % LANES
    return pltpu.roll(group, shift, 1) if shift else group


def halo_kernel(
    container_ref, ext0, ext1, ext2, ext3, row_send, row_recv, col_send, col_recv, send_sem, recv_sem
):
    level = lax.axis_index("branch")
    place = lax.axis_index("row")
    col = lax.axis_index("col")
    row_count = lax.axis_size("row")
    col_count = lax.axis_size("col")
    up, down = place > 0, place < row_count - 1
    left, right = col > 0, col < col_count - 1
    above = (level, lax.rem(place + row_count - 1, row_count), col)
    below = (level, lax.rem(place + 1, row_count), col)
    west = (level, place, lax.rem(col + col_count - 1, col_count))
    east = (level, place, lax.rem(col + 1, col_count))
    neighbours = ((up, above), (down, below), (left, west), (right, east))

    barrier = pltpu.get_barrier_semaphore()
    for exists, device in neighbours:

        @pl.when(exists)
        def _():
            pl.semaphore_signal(barrier, inc=1, device_id=device, device_id_type=MESH)

    pl.semaphore_wait(barrier, sum(exists.astype(jnp.int32) for exists, _ in neighbours))

    def side_copy(rows, way):
        source, target = (row_send, row_recv) if way < 2 else (col_send, col_recv)
        return pltpu.make_async_remote_copy(
            src_ref=source.at[way % 2, 0:rows],
            dst_ref=target.at[1 - way % 2, 0:rows],
            send_sem=send_sem.at[way],
            recv_sem=recv_sem.at[way],
            device_id=neighbours[way][1],
            device_id_type=MESH,
        )

    lane = lax.broadcasted_iota(jnp.int32, (1, LANES), 1)

    def swap(rows, first_way):
        for way in (first_way, first_way + 1):

            @pl.when(neighbours[way][0])
            def _():
                side_copy(rows, way).start()

        received = row_recv if first_way == 0 else col_recv
        for way in (first_way, first_way + 1):
            exists = neighbours[first_way + 1 - way % 2][0]

            @pl.when(exists)
            def _():
                side_copy(rows, way).wait_recv()

            @pl.when(jnp.logical_not(exists))
            def _():
                received[1 - way % 2, 0:rows] = jnp.zeros((rows, LANES), jnp.bfloat16)

    def extend(branch_level, out_ref):
        channels, total = out_ref.shape
        rows, cols, pitch = TH >> branch_level, TW >> branch_level, row_pitch(branch_level)
        apart = cols * 2 >= LANES
        tile = natural_tile(branch_level, container_ref)

        def tile_row(y):
            at = y * cols
            low = at // LANES * LANES
            return tile[:, low : low + LANES], at - low

        for side, first in enumerate((0, rows - 2)):
            if apart:
                for turn in range(2):
                    group, at = tile_row(first + turn)
                    row_send[side, turn * channels : (turn + 1) * channels] = turned(
                        group, -at
                    ).astype(jnp.bfloat16)
            else:
                group, at = tile_row(first)
                row_send[side, 0:channels] = turned(group, -at).astype(jnp.bfloat16)
        swap(2 * channels if apart else channels, 0)

        def wide_row(r):
            if 2 <= r < rows + 2:
                return tile_row(r - 2)
            side, turn = (0, r) if r < 2 else (1, r - rows - 2)
            if apart:
                group = row_recv[side, turn * channels : (turn + 1) * channels]
                return group.astype(jnp.float32), 0
            return row_recv[side, 0:channels].astype(jnp.float32), turn * cols

        firsts = jnp.zeros((channels, LANES), jnp.float32)
        lasts = firsts
        for r in range(rows + 4):
            group, at = wide_row(r)
            here = lax.shift_right_logical(lane, 1) == r
            firsts = jnp.where(here, turned(group, 2 * r - at), firsts)
            lasts = jnp.where(here, turned(group, 2 * r - at - cols + 2), lasts)
        col_send[0, 0:channels] = firsts.astype(jnp.bfloat16)
        col_send[1, 0:channels] = lasts.astype(jnp.bfloat16)
        swap(channels, 2)
        from_west = col_recv[0, 0:channels].astype(jnp.float32)
        from_east = col_recv[1, 0:channels].astype(jnp.float32)

        groups = [None] * (total // LANES)

        def put(start, count, group, at):
            index, low = start // LANES, start % LANES
            group = turned(group, low - at)
            held = 0.0 if groups[index] is None else groups[index]
            groups[index] = (
                group
                if count == LANES
                else jnp.where((lane >= low) & (lane < low + count), group, held)
            )

        for r in range(rows + 4):
            put(r * pitch, cols, *wide_row(r))
            put(r * pitch + cols, 2, from_east, 2 * r)
            put((r - 1) % (rows + 4) * pitch + pitch - 2, 2, from_west, 2 * r)
        for index, group in enumerate(groups):
            out_ref[:, index * LANES : (index + 1) * LANES] = group.astype(jnp.bfloat16)

        for first_way, count in ((0, 2 * channels if apart else channels), (2, channels)):
            for way in (first_way, first_way + 1):

                @pl.when(neighbours[way][0])
                def _():
                    side_copy(count, way).wait_send()

    for branch_level, out_ref in enumerate((ext0, ext1, ext2, ext3)):
        pl.when(level == branch_level)(partial(extend, branch_level, out_ref))


def extended_tiles(container):
    vmem = pl.BlockSpec(memory_space=pltpu.VMEM)
    side = pltpu.VMEM((2, 8 * WIDTH, LANES), jnp.bfloat16)
    return pl.pallas_call(
        halo_kernel,
        out_shape=[
            jax.ShapeDtypeStruct((WIDTH << b, ((TH >> b) + 4) * row_pitch(b)), jnp.bfloat16)
            for b in range(4)
        ],
        in_specs=[vmem],
        out_specs=[vmem] * 4,
        scratch_shapes=[
            side,
            side,
            side,
            side,
            pltpu.SemaphoreType.DMA((4,)),
            pltpu.SemaphoreType.DMA((4,)),
        ],
        compiler_params=pltpu.CompilerParams(collective_id=1, has_side_effects=True),
        name="halo",
    )(container)


def tap_stack(field, pitch, rows_kept):
    total = field.shape[1]
    views = {}
    for dx in (-1, 0, 1):
        if pitch % LANES == 0:
            view = field if dx == 0 else pltpu.roll(field, -dx % total, 1)
            view = view.astype(jnp.bfloat16)
            if rows_kept:
                step = LANES
                view = jnp.concatenate(
                    [view[:, y * pitch : y * pitch + LANES] for y in range(1, rows_kept + 3)],
                    axis=1,
                )
                size = rows_kept * LANES
            else:
                step = pitch
                view = jnp.concatenate([view[:, total - pitch :], view, view[:, :pitch]], axis=1)
                size = total
            for dy in range(3):
                views[dy, dx] = view[:, dy * step : dy * step + size]
        else:
            for dy in range(3):
                shift = -(dx + (dy - 1) * pitch) % total
                view = field if shift == 0 else pltpu.roll(field, shift, 1)
                views[dy, dx] = view.astype(jnp.bfloat16)
    return jnp.concatenate([views[dy, dx] for dy in range(3) for dx in (-1, 0, 1)], axis=0)


def taps_of(weight_ref):
    if len(weight_ref.shape) == 2:
        return weight_ref[...]
    return jnp.concatenate([weight_ref[dy, dx] for dy in range(3) for dx in range(3)], axis=1)


def block_kernel(branch_level, ext_ref, first_ref, second_ref, bias_ref, strips_ref):
    pitch = row_pitch(branch_level)
    tile_rows, tile_cols = TH >> branch_level, TW >> branch_level
    channels, total = ext_ref.shape
    place, col = lax.axis_index("row"), lax.axis_index("col")
    field = ext_ref[...].astype(jnp.float32)
    first, second = taps_of(first_ref), taps_of(second_ref)
    hidden = jnp.dot(first, tap_stack(field, pitch, 0), preferred_element_type=jnp.float32)
    hidden = jnp.maximum(hidden + bias_ref[0], 0.0)
    pixel = lax.broadcasted_iota(jnp.int32, (1, total), 1) + 1
    y = lax.shift_right_logical(pixel, pitch.bit_length() - 1)
    x = pixel & (pitch - 1)
    top = jnp.where(place == 0, 1, -1)
    bottom = jnp.where(place == lax.axis_size("row") - 1, tile_rows + 2, -1)
    left = jnp.where(col == 0, 0, -1)
    right = jnp.where(col == lax.axis_size("col") - 1, tile_cols + 1, -1)
    inside = (y != top) & (y != bottom) & (x != left) & (x != right)
    hidden = jnp.where(inside, hidden, 0.0).astype(jnp.bfloat16).astype(jnp.float32)
    narrow = tile_cols == LANES
    rows_kept = tile_rows if narrow else 0
    after = jnp.dot(
        second, tap_stack(hidden, pitch, rows_kept), preferred_element_type=jnp.float32
    )
    if narrow:
        field = jnp.concatenate(
            [field[:, y * pitch : y * pitch + LANES] for y in range(2, tile_rows + 2)], axis=1
        )
    settled = jnp.maximum(after + bias_ref[1] + field, 0.0)
    strip_rows = tile_rows // STRIPS
    lane = lax.broadcasted_iota(jnp.int32, (1, LANES), 1)
    for strip in range(STRIPS):
        groups = []
        if narrow:
            groups = [
                settled[:, y * LANES : (y + 1) * LANES]
                for y in range(strip * strip_rows, (strip + 1) * strip_rows)
            ]
        else:
            per_group = min(LANES // tile_cols, strip_rows)
            for start in range(0, strip_rows, per_group):
                merged = None
                for turn in range(per_group):
                    at = (strip * strip_rows + start + turn + 2) * pitch
                    part = settled[:, at // LANES * LANES : at // LANES * LANES + LANES]
                    shift = (turn * tile_cols - at) % LANES
                    part = pltpu.roll(part, shift, 1) if shift else part
                    merged = part if turn == 0 else jnp.where(lane < turn * tile_cols, merged, part)
                groups.append(merged)
        for at, group in enumerate(groups):
            strips_ref[strip, at * channels : (at + 1) * channels] = group.astype(jnp.bfloat16)


def deep_block(branch_level, tiles, kernels, biases):
    channels = WIDTH << branch_level
    extended = tiles[branch_level]
    if channels == kernels.shape[-1] and channels % LANES == 0:
        first, second = kernels[0], kernels[1]
    else:
        first, second = (
            jnp.concatenate(
                [
                    kernels[layer, dy, dx, :channels, :channels]
                    for dy in range(3)
                    for dx in range(3)
                ],
                axis=1,
            )
            for layer in range(2)
        )
    vmem = pl.BlockSpec(memory_space=pltpu.VMEM)
    return pl.pallas_call(
        partial(block_kernel, branch_level),
        out_shape=jax.ShapeDtypeStruct((STRIPS, PIECE_ROWS, LANES), jnp.bfloat16),
        in_specs=[vmem] * 4,
        out_specs=vmem,
        compiler_params=pltpu.CompilerParams(vmem_limit_bytes=60 << 20),
        name=f"block_{branch_level}",
    )(extended, first, second, biases[:, :channels, None])


LANES = 128
STRIPS = 4
PIECE_ROWS = WIDTH * TH * TW // (STRIPS * LANES)
MESH = pl.DeviceIdType.MESH


def piece_rows(branch_level):
    pixels = TH * TW // STRIPS >> 2 * branch_level
    return (WIDTH << branch_level) * max(1, pixels // LANES)


def block_mask(fine_level, coarse_level):
    fine_cols = TW >> fine_level
    coarse_cols = TW >> coarse_level
    fine = TH * TW // STRIPS >> 2 * fine_level
    coarse = TH * TW // STRIPS >> 2 * coarse_level
    shift = coarse_level - fine_level
    pixel = lax.broadcasted_iota(jnp.int32, (fine, 1), 0)
    row = lax.shift_right_logical(pixel, fine_cols.bit_length() - 1 + shift)
    col = lax.shift_right_logical(pixel & (fine_cols - 1), shift)
    home = row * coarse_cols + col
    target = lax.broadcasted_iota(jnp.int32, (fine, coarse), 1)
    return jnp.where(home == target, 1.0, 0.0).astype(jnp.bfloat16)


def mixed(weight_ref, target, source, tile_data):
    start = ((1 << source) - 1) * WIDTH
    low = start // LANES * LANES
    high = min(-(-(start + tile_data.shape[0]) // LANES) * LANES, weight_ref.shape[1])
    pieces = []
    if start > low:
        pieces.append(jnp.zeros((start - low, tile_data.shape[1]), tile_data.dtype))
    pieces.append(tile_data)
    if high > start + tile_data.shape[0]:
        pieces.append(
            jnp.zeros((high - start - tile_data.shape[0], tile_data.shape[1]), tile_data.dtype)
        )
    rows = ((1 << target) - 1) * WIDTH
    return jnp.dot(
        weight_ref[rows : rows + (WIDTH << target), low:high],
        jnp.concatenate(pieces, axis=0),
        preferred_element_type=jnp.float32,
    ).astype(jnp.bfloat16)


def join_strip(maps, masks, weight_ref, bias_ref, out_refs):
    for target in range(4):
        start = ((1 << target) - 1) * WIDTH
        total = maps[target].astype(jnp.float32) + bias_ref[start : start + (WIDTH << target), :]
        for source in range(4):
            if source < target:
                share = 0.25 ** (target - source)
                shrunk = jnp.dot(
                    maps[source], masks[source, target], preferred_element_type=jnp.float32
                )
                term = mixed(weight_ref, target, source, (shrunk * share).astype(jnp.bfloat16))
                total = total + term.astype(jnp.float32)
            elif source > target:
                term = mixed(weight_ref, target, source, maps[source])
                total = total + lax.dot_general(
                    term,
                    masks[target, source],
                    (((1,), (1,)), ((), ())),
                    preferred_element_type=jnp.float32,
                )
        out_refs[target][...] = jnp.maximum(total, 0.0).astype(jnp.bfloat16)


def exchange_join(
    strips_ref, weight_ref, bias_ref, out0, out1, out2, out3, held, send_sem, recv_sem, own_sem
):
    level = lax.axis_index("branch")
    place = lax.axis_index("row")
    col = lax.axis_index("col")
    home = level == place

    barrier = pltpu.get_barrier_semaphore()
    for other in range(4):

        @pl.when(jnp.logical_not(home & (level == other)))
        def _():
            pl.semaphore_signal(
                barrier, inc=1, device_id=(other, level, col), device_id_type=MESH
            )

    pl.semaphore_wait(barrier, jnp.where(home, 3, 4))

    def remote(source, strip):
        rows = piece_rows(source)
        return pltpu.make_async_remote_copy(
            src_ref=strips_ref.at[strip, 0:rows],
            dst_ref=held.at[source, 0:rows],
            send_sem=send_sem.at[strip],
            recv_sem=recv_sem.at[source],
            device_id=(place, strip, col),
            device_id_type=MESH,
        )

    def own(source):
        rows = piece_rows(source)
        return pltpu.make_async_copy(
            strips_ref.at[source, 0:rows], held.at[source, 0:rows], own_sem
        )

    for source in range(4):
        for step in range(4):
            strip = (source + 1 + step) % 4

            @pl.when((level == source) & jnp.logical_not(home & (level == strip)))
            def _():
                remote(source, strip).start()

        @pl.when((level == source) & home)
        def _():
            own(source).start()

    masks = {
        (fine, coarse): block_mask(fine, coarse)
        for fine in range(3)
        for coarse in range(fine + 1, 4)
    }

    for source in range(4):

        @pl.when(jnp.logical_not(home & (level == source)))
        def _():
            remote(source, 0).wait_recv()

        @pl.when((level == source) & home)
        def _():
            own(source).wait()

    maps = []
    for source in range(4):
        channels = WIDTH << source
        pixels = TH * TW // STRIPS >> 2 * source
        if pixels >= LANES:
            maps.append(
                jnp.concatenate(
                    [
                        held[source, at * channels : (at + 1) * channels]
                        for at in range(pixels // LANES)
                    ],
                    axis=1,
                )
            )
        else:
            maps.append(held[source, 0:channels][:, :pixels])
    join_strip(maps, masks, weight_ref, bias_ref, (out0, out1, out2, out3))

    for source in range(4):
        for strip in range(4):

            @pl.when((level == source) & jnp.logical_not(home & (level == strip)))
            def _():
                remote(source, strip).wait_send()


def joined(strips, join_weight, join_bias):
    vmem = pl.BlockSpec(memory_space=pltpu.VMEM)
    return pl.pallas_call(
        exchange_join,
        out_shape=[
            jax.ShapeDtypeStruct(
                (WIDTH << b, TH * TW // STRIPS >> 2 * b), jnp.bfloat16
            )
            for b in range(4)
        ],
        in_specs=[vmem] * 3,
        out_specs=[vmem] * 4,
        scratch_shapes=[
            pltpu.VMEM((4, PIECE_ROWS, LANES), jnp.bfloat16),
            pltpu.SemaphoreType.DMA((4,)),
            pltpu.SemaphoreType.DMA((4,)),
            pltpu.SemaphoreType.DMA,
        ],
        compiler_params=pltpu.CompilerParams(collective_id=0, has_side_effects=True),
        name="exchange_join",
    )(strips, join_weight, join_bias[:, None])


def local(section_in, conv_weight, conv_bias, join_weight, join_bias):
    level_index = lax.axis_index("branch")
    container = section_in[0, 0, 0]
    kernels = conv_weight[0]
    biases = conv_bias[0]
    tiles = extended_tiles(container)
    strips = lax.switch(
        level_index,
        [partial(deep_block, branch_level) for branch_level in range(4)],
        tiles,
        kernels,
        biases,
    )
    outs = joined(strips, join_weight, join_bias)
    return tuple(
        out.reshape(WIDTH << b, (TH >> b) // STRIPS, TW >> b) for b, out in enumerate(outs)
    )


def solution(mesh):
    in_specs = (
        P("branch", "row", "col", None, None),
        P("branch", None, None, None, None, None),
        P("branch", None, None),
        P(),
        P(),
    )
    out_specs = (
        P(None, ("branch", "row"), "col"),
        P(None, ("branch", "row"), "col"),
        P(None, ("branch", "row"), "col"),
        P(None, ("branch", "row"), "col"),
    )
    return jax.shard_map(local, mesh=mesh, in_specs=in_specs, out_specs=out_specs, check_vma=False)
```

```python
from functools import partial

import jax
import jax.numpy as jnp
from jax import lax
from jax.experimental import pallas as pl
from jax.experimental.pallas import tpu as pltpu
from jax.sharding import PartitionSpec as P

WIDTH = 48
TH = 32
TW = 128


def row_pitch(branch_level):
    return 2 * TW >> branch_level


def natural_tile(branch_level, container_ref):
    pixels = TH * TW >> 2 * branch_level
    if branch_level == 0:
        return container_ref[...].astype(jnp.float32)
    channels = WIDTH << branch_level
    parts = []
    for part in range(1 << branch_level):
        at = part * pixels
        low = at // LANES * LANES
        piece = container_ref[:, low : low + max(pixels, LANES)]
        if at > low:
            piece = pltpu.roll(piece.astype(jnp.float32), LANES - at + low, 1).astype(jnp.bfloat16)
        parts.append(piece)
    held = lax.broadcasted_iota(jnp.int32, (1, channels), 1)
    part = sum((held >= WIDTH * turn).astype(jnp.int32) for turn in range(1, 1 << branch_level))
    home = ((held - WIDTH * part) << branch_level) + part
    order = jnp.where(lax.broadcasted_iota(jnp.int32, (channels, channels), 0) == home, 1.0, 0.0)
    return jnp.dot(
        order.astype(jnp.bfloat16),
        jnp.concatenate(parts, axis=0),
        preferred_element_type=jnp.float32,
    )


def turned(group, shift):
    shift = shift % LANES
    return pltpu.roll(group, shift, 1) if shift else group


def halo_kernel(
    container_ref, ext0, ext1, ext2, ext3, row_send, row_recv, col_send, col_recv, send_sem, recv_sem
):
    level = lax.axis_index("branch")
    place = lax.axis_index("row")
    col = lax.axis_index("col")
    row_count = lax.axis_size("row")
    col_count = lax.axis_size("col")
    up, down = place > 0, place < row_count - 1
    left, right = col > 0, col < col_count - 1
    above = (level, lax.rem(place + row_count - 1, row_count), col)
    below = (level, lax.rem(place + 1, row_count), col)
    west = (level, place, lax.rem(col + col_count - 1, col_count))
    east = (level, place, lax.rem(col + 1, col_count))
    neighbours = ((up, above), (down, below), (left, west), (right, east))

    barrier = pltpu.get_barrier_semaphore()
    for exists, device in neighbours:

        @pl.when(exists)
        def _():
            pl.semaphore_signal(barrier, inc=1, device_id=device, device_id_type=MESH)

    pl.semaphore_wait(barrier, sum(exists.astype(jnp.int32) for exists, _ in neighbours))

    def side_copy(rows, way):
        source, target = (row_send, row_recv) if way < 2 else (col_send, col_recv)
        return pltpu.make_async_remote_copy(
            src_ref=source.at[way % 2, 0:rows],
            dst_ref=target.at[1 - way % 2, 0:rows],
            send_sem=send_sem.at[way],
            recv_sem=recv_sem.at[way],
            device_id=neighbours[way][1],
            device_id_type=MESH,
        )

    lane = lax.broadcasted_iota(jnp.int32, (1, LANES), 1)

    def swap(rows, first_way):
        for way in (first_way, first_way + 1):

            @pl.when(neighbours[way][0])
            def _():
                side_copy(rows, way).start()

        received = row_recv if first_way == 0 else col_recv
        for way in (first_way, first_way + 1):
            exists = neighbours[first_way + 1 - way % 2][0]

            @pl.when(exists)
            def _():
                side_copy(rows, way).wait_recv()

            @pl.when(jnp.logical_not(exists))
            def _():
                received[1 - way % 2, 0:rows] = jnp.zeros((rows, LANES), jnp.bfloat16)

    def extend(branch_level, out_ref):
        channels, total = out_ref.shape
        rows, cols, pitch = TH >> branch_level, TW >> branch_level, row_pitch(branch_level)
        apart = cols * 2 >= LANES
        tile = natural_tile(branch_level, container_ref)

        def tile_row(y):
            at = y * cols
            low = at // LANES * LANES
            return tile[:, low : low + LANES], at - low

        for side, first in enumerate((0, rows - 2)):
            if apart:
                for turn in range(2):
                    group, at = tile_row(first + turn)
                    row_send[side, turn * channels : (turn + 1) * channels] = turned(
                        group, -at
                    ).astype(jnp.bfloat16)
            else:
                group, at = tile_row(first)
                row_send[side, 0:channels] = turned(group, -at).astype(jnp.bfloat16)
        swap(2 * channels if apart else channels, 0)

        def wide_row(r):
            if 2 <= r < rows + 2:
                return tile_row(r - 2)
            side, turn = (0, r) if r < 2 else (1, r - rows - 2)
            if apart:
                group = row_recv[side, turn * channels : (turn + 1) * channels]
                return group.astype(jnp.float32), 0
            return row_recv[side, 0:channels].astype(jnp.float32), turn * cols

        firsts = jnp.zeros((channels, LANES), jnp.float32)
        lasts = firsts
        for r in range(rows + 4):
            group, at = wide_row(r)
            here = lax.shift_right_logical(lane, 1) == r
            firsts = jnp.where(here, turned(group, 2 * r - at), firsts)
            lasts = jnp.where(here, turned(group, 2 * r - at - cols + 2), lasts)
        col_send[0, 0:channels] = firsts.astype(jnp.bfloat16)
        col_send[1, 0:channels] = lasts.astype(jnp.bfloat16)
        swap(channels, 2)
        from_west = col_recv[0, 0:channels].astype(jnp.float32)
        from_east = col_recv[1, 0:channels].astype(jnp.float32)

        groups = [None] * (total // LANES)

        def put(start, count, group, at):
            index, low = start // LANES, start % LANES
            group = turned(group, low - at)
            held = 0.0 if groups[index] is None else groups[index]
            groups[index] = (
                group
                if count == LANES
                else jnp.where((lane >= low) & (lane < low + count), group, held)
            )

        for r in range(rows + 4):
            put(r * pitch, cols, *wide_row(r))
            put(r * pitch + cols, 2, from_east, 2 * r)
            put((r - 1) % (rows + 4) * pitch + pitch - 2, 2, from_west, 2 * r)
        for index, group in enumerate(groups):
            out_ref[:, index * LANES : (index + 1) * LANES] = group.astype(jnp.bfloat16)

        for first_way, count in ((0, 2 * channels if apart else channels), (2, channels)):
            for way in (first_way, first_way + 1):

                @pl.when(neighbours[way][0])
                def _():
                    side_copy(count, way).wait_send()

    for branch_level, out_ref in enumerate((ext0, ext1, ext2, ext3)):
        pl.when(level == branch_level)(partial(extend, branch_level, out_ref))


def extended_tiles(container):
    vmem = pl.BlockSpec(memory_space=pltpu.VMEM)
    side = pltpu.VMEM((2, 8 * WIDTH, LANES), jnp.bfloat16)
    return pl.pallas_call(
        halo_kernel,
        out_shape=[
            jax.ShapeDtypeStruct((WIDTH << b, ((TH >> b) + 4) * row_pitch(b)), jnp.bfloat16)
            for b in range(4)
        ],
        in_specs=[vmem],
        out_specs=[vmem] * 4,
        scratch_shapes=[
            side,
            side,
            side,
            side,
            pltpu.SemaphoreType.DMA((4,)),
            pltpu.SemaphoreType.DMA((4,)),
        ],
        compiler_params=pltpu.CompilerParams(collective_id=1, has_side_effects=True),
        name="halo",
    )(container)


def tap_stack(field, pitch, rows_kept):
    total = field.shape[1]
    views = {}
    for dx in (-1, 0, 1):
        if pitch % LANES == 0:
            view = field if dx == 0 else pltpu.roll(field, -dx % total, 1)
            view = view.astype(jnp.bfloat16)
            if rows_kept:
                step = LANES
                view = jnp.concatenate(
                    [view[:, y * pitch : y * pitch + LANES] for y in range(1, rows_kept + 3)],
                    axis=1,
                )
                size = rows_kept * LANES
            else:
                step = pitch
                view = jnp.concatenate([view[:, total - pitch :], view, view[:, :pitch]], axis=1)
                size = total
            for dy in range(3):
                views[dy, dx] = view[:, dy * step : dy * step + size]
        else:
            for dy in range(3):
                shift = -(dx + (dy - 1) * pitch) % total
                view = field if shift == 0 else pltpu.roll(field, shift, 1)
                views[dy, dx] = view.astype(jnp.bfloat16)
    return jnp.concatenate([views[dy, dx] for dy in range(3) for dx in (-1, 0, 1)], axis=0)


def taps_of(weight_refs, layer):
    if len(weight_refs) == 2:
        return weight_refs[layer][...]
    (weight_ref,) = weight_refs
    return jnp.concatenate(
        [weight_ref[layer, dy, dx] for dy in range(3) for dx in range(3)], axis=1
    )


def folded(group, pixels):
    folds = LANES // pixels
    size = group.shape[0] // folds
    lane = lax.broadcasted_iota(jnp.int32, (1, LANES), 1)
    merged = group[:size]
    for turn in range(1, folds):
        part = turned(group[turn * size : (turn + 1) * size], turn * pixels)
        merged = jnp.where(lane < turn * pixels, merged, part)
    return [merged]


def block_kernel(branch_level, ext_ref, bias_ref, *refs):
    weight_refs, strips_ref = refs[:-1], refs[-1]
    pitch = row_pitch(branch_level)
    tile_rows, tile_cols = TH >> branch_level, TW >> branch_level
    channels, total = ext_ref.shape
    place, col = lax.axis_index("row"), lax.axis_index("col")
    field = ext_ref[...].astype(jnp.float32)
    first, second = taps_of(weight_refs, 0), taps_of(weight_refs, 1)
    hidden = jnp.dot(first, tap_stack(field, pitch, 0), preferred_element_type=jnp.float32)
    hidden = jnp.maximum(hidden + bias_ref[0], 0.0)
    pixel = lax.broadcasted_iota(jnp.int32, (1, total), 1) + 1
    y = lax.shift_right_logical(pixel, pitch.bit_length() - 1)
    x = pixel & (pitch - 1)
    top = jnp.where(place == 0, 1, -1)
    bottom = jnp.where(place == lax.axis_size("row") - 1, tile_rows + 2, -1)
    left = jnp.where(col == 0, 0, -1)
    right = jnp.where(col == lax.axis_size("col") - 1, tile_cols + 1, -1)
    inside = (y != top) & (y != bottom) & (x != left) & (x != right)
    hidden = jnp.where(inside, hidden, 0.0).astype(jnp.bfloat16).astype(jnp.float32)
    narrow = tile_cols == LANES
    rows_kept = tile_rows if narrow else 0
    after = jnp.dot(
        second, tap_stack(hidden, pitch, rows_kept), preferred_element_type=jnp.float32
    )
    if narrow:
        field = jnp.concatenate(
            [field[:, y * pitch : y * pitch + LANES] for y in range(2, tile_rows + 2)], axis=1
        )
    settled = jnp.maximum(after + bias_ref[1] + field, 0.0)
    strip_rows = tile_rows // STRIPS
    lane = lax.broadcasted_iota(jnp.int32, (1, LANES), 1)
    for strip in range(STRIPS):
        groups = []
        if narrow:
            groups = [
                settled[:, y * LANES : (y + 1) * LANES]
                for y in range(strip * strip_rows, (strip + 1) * strip_rows)
            ]
        else:
            per_group = min(LANES // tile_cols, strip_rows)
            for start in range(0, strip_rows, per_group):
                merged = None
                for turn in range(per_group):
                    at = (strip * strip_rows + start + turn + 2) * pitch
                    part = settled[:, at // LANES * LANES : at // LANES * LANES + LANES]
                    shift = (turn * tile_cols - at) % LANES
                    part = pltpu.roll(part, shift, 1) if shift else part
                    merged = part if turn == 0 else jnp.where(lane < turn * tile_cols, merged, part)
                groups.append(merged)
        if len(groups) == 1:
            groups = folded(groups[0], strip_rows * tile_cols)
        size = groups[0].shape[0]
        for at, group in enumerate(groups):
            strips_ref[strip, at * size : (at + 1) * size] = group.astype(jnp.bfloat16)


def deep_block(branch_level, tiles, kernels, biases):
    channels = WIDTH << branch_level
    extended = tiles[branch_level]
    if channels == kernels.shape[-1] and channels % LANES == 0:
        weights = [kernels]
    else:
        weights = [
            jnp.concatenate(
                [
                    kernels[layer, dy, dx, :channels, :channels]
                    for dy in range(3)
                    for dx in range(3)
                ],
                axis=1,
            )
            for layer in range(2)
        ]
    vmem = pl.BlockSpec(memory_space=pltpu.VMEM)
    return pl.pallas_call(
        partial(block_kernel, branch_level),
        out_shape=jax.ShapeDtypeStruct((STRIPS, PIECE_ROWS, LANES), jnp.bfloat16),
        in_specs=[vmem] * (2 + len(weights)),
        out_specs=vmem,
        compiler_params=pltpu.CompilerParams(vmem_limit_bytes=60 << 20),
        name=f"block_{branch_level}",
    )(extended, biases[:, :channels, None], *weights)


LANES = 128
STRIPS = 4
PIECE_ROWS = WIDTH * TH * TW // (STRIPS * LANES)
MESH = pl.DeviceIdType.MESH


def piece_rows(branch_level):
    return PIECE_ROWS >> branch_level


def block_mask(fine_level, coarse_level):
    fine_cols = TW >> fine_level
    coarse_cols = TW >> coarse_level
    fine = TH * TW // STRIPS >> 2 * fine_level
    coarse = TH * TW // STRIPS >> 2 * coarse_level
    shift = coarse_level - fine_level
    pixel = lax.broadcasted_iota(jnp.int32, (fine, 1), 0)
    row = lax.shift_right_logical(pixel, fine_cols.bit_length() - 1 + shift)
    col = lax.shift_right_logical(pixel & (fine_cols - 1), shift)
    home = row * coarse_cols + col
    target = lax.broadcasted_iota(jnp.int32, (fine, coarse), 1)
    return jnp.where(home == target, 1.0, 0.0).astype(jnp.bfloat16)


def mixed(weight_ref, target, source, tile_data):
    start = ((1 << source) - 1) * WIDTH
    low = start // LANES * LANES
    high = min(-(-(start + tile_data.shape[0]) // LANES) * LANES, weight_ref.shape[1])
    pieces = []
    if start > low:
        pieces.append(jnp.zeros((start - low, tile_data.shape[1]), tile_data.dtype))
    pieces.append(tile_data)
    if high > start + tile_data.shape[0]:
        pieces.append(
            jnp.zeros((high - start - tile_data.shape[0], tile_data.shape[1]), tile_data.dtype)
        )
    rows = ((1 << target) - 1) * WIDTH
    return jnp.dot(
        weight_ref[rows : rows + (WIDTH << target), low:high],
        jnp.concatenate(pieces, axis=0),
        preferred_element_type=jnp.float32,
    ).astype(jnp.bfloat16)


def join_strip(maps, masks, weight_ref, bias_ref, out_refs):
    for target in range(4):
        start = ((1 << target) - 1) * WIDTH
        total = maps[target].astype(jnp.float32) + bias_ref[start : start + (WIDTH << target), :]
        for source in range(4):
            if source < target:
                share = 0.25 ** (target - source)
                shrunk = jnp.dot(
                    maps[source], masks[source, target], preferred_element_type=jnp.float32
                )
                term = mixed(weight_ref, target, source, (shrunk * share).astype(jnp.bfloat16))
                total = total + term.astype(jnp.float32)
            elif source > target:
                term = mixed(weight_ref, target, source, maps[source])
                total = total + lax.dot_general(
                    term,
                    masks[target, source],
                    (((1,), (1,)), ((), ())),
                    preferred_element_type=jnp.float32,
                )
        total = jnp.maximum(total, 0.0)
        out_ref = out_refs[target]
        if len(out_ref.shape) == 2:
            out_ref[...] = total.T.astype(jnp.bfloat16)
        else:
            lines = [total[:, at : at + LANES] for at in range(0, total.shape[1], LANES)]
            out_ref[...] = jnp.stack(lines, axis=1).astype(jnp.bfloat16)


def exchange_kernel(
    strips_ref, held, relay, near_send, near_recv, far_send, far_recv, own_sem
):
    level = lax.axis_index("branch")
    place = lax.axis_index("row")
    col = lax.axis_index("col")
    size = STRIPS
    home = level == place

    barrier = pltpu.get_barrier_semaphore()
    for step in range(1, size):
        for device in (
            (level, lax.rem(place + step, size), col),
            (lax.rem(level + step, size), place, col),
        ):
            pl.semaphore_signal(barrier, inc=1, device_id=device, device_id_type=MESH)
    pl.semaphore_wait(barrier, 2 * (size - 1))

    def near(rows, step):
        strip = lax.rem(place + step, size)
        return pltpu.make_async_remote_copy(
            src_ref=strips_ref.at[strip, 0:rows],
            dst_ref=relay.at[step - 1, 0:rows],
            send_sem=near_send.at[step - 1],
            recv_sem=near_recv.at[step - 1],
            device_id=(level, strip, col),
            device_id_type=MESH,
        )

    def far(source, step):
        rows = piece_rows(source)
        tile = lax.rem(place + size - step, size)
        piece = strips_ref.at[place, 0:rows] if step == 0 else relay.at[step - 1, 0:rows]
        return (
            tile,
            pltpu.make_async_remote_copy(
                src_ref=piece,
                dst_ref=held.at[source, 0:rows],
                send_sem=far_send.at[step],
                recv_sem=far_recv.at[source],
                device_id=(tile, place, col),
                device_id_type=MESH,
            ),
            pltpu.make_async_copy(piece, held.at[source, 0:rows], own_sem),
        )

    def onward(source):
        rows = piece_rows(source)
        for step in (2, 1, 3):
            near(rows, step).start()
        for step in (0, 1, 3, 2):
            if step:
                near(rows, step).wait_recv()
            tile, remote, own = far(source, step)
            pl.when(tile != level)(remote.start)
            pl.when(tile == level)(own.start)

    for source in range(size):
        pl.when(level == source)(partial(onward, source))

    for source in range(size):
        _, remote, own = far(source, 0)
        pl.when(level != source)(remote.wait_recv)
        pl.when(level == source)(own.wait)

    def sent(source):
        for step in range(1, size):
            near(piece_rows(source), step).wait_send()
        for step in range(size):
            tile, remote, _ = far(source, step)
            pl.when(tile != level)(remote.wait_send)

    for source in range(size):
        pl.when(level == source)(partial(sent, source))


def join_kernel(held, weight_ref, bias_ref, *out_refs):
    masks = {
        (fine, coarse): block_mask(fine, coarse)
        for fine in range(3)
        for coarse in range(fine + 1, 4)
    }
    maps = []
    for source in range(4):
        channels = WIDTH << source
        pixels = TH * TW // STRIPS >> 2 * source
        if pixels >= LANES:
            maps.append(
                jnp.concatenate(
                    [
                        held[source, at * channels : (at + 1) * channels]
                        for at in range(pixels // LANES)
                    ],
                    axis=1,
                )
            )
        else:
            piece = held[source, 0 : piece_rows(source)].astype(jnp.float32)
            unfolded = jnp.concatenate(
                [turned(piece, -turn * pixels) for turn in range(LANES // pixels)], axis=0
            )
            maps.append(unfolded.astype(jnp.bfloat16)[:, :pixels])
    join_strip(maps, masks, weight_ref, bias_ref, out_refs)


def joined(strips, join_weight, join_bias):
    vmem = pl.BlockSpec(memory_space=pltpu.VMEM)
    held = pl.pallas_call(
        exchange_kernel,
        out_shape=jax.ShapeDtypeStruct((STRIPS, PIECE_ROWS, LANES), jnp.bfloat16),
        in_specs=[vmem],
        out_specs=vmem,
        scratch_shapes=[
            pltpu.VMEM((STRIPS - 1, PIECE_ROWS, LANES), jnp.bfloat16),
            pltpu.SemaphoreType.DMA((STRIPS - 1,)),
            pltpu.SemaphoreType.DMA((STRIPS - 1,)),
            pltpu.SemaphoreType.DMA((STRIPS,)),
            pltpu.SemaphoreType.DMA((STRIPS,)),
            pltpu.SemaphoreType.DMA,
        ],
        compiler_params=pltpu.CompilerParams(collective_id=0, has_side_effects=True),
        name="exchange",
    )(strips)
    shapes = [(WIDTH << b, (TH >> b) // STRIPS, TW >> b) for b in range(4)]
    outs = pl.pallas_call(
        join_kernel,
        out_shape=[
            jax.ShapeDtypeStruct(
                shape if shape[2] == LANES else (shape[1] * shape[2], shape[0]), jnp.bfloat16
            )
            for shape in shapes
        ],
        in_specs=[vmem] * 3,
        out_specs=[vmem] * 4,
        name="join",
    )(held, join_weight, join_bias[:, None])
    return tuple(
        out if out.ndim == 3 else out.reshape(*shape[1:], shape[0]).transpose(2, 0, 1)
        for out, shape in zip(outs, shapes)
    )


def local(section_in, conv_weight, conv_bias, join_weight, join_bias):
    level_index = lax.axis_index("branch")
    container = section_in[0, 0, 0]
    kernels = conv_weight[0]
    biases = conv_bias[0]
    tiles = extended_tiles(container)
    strips = lax.switch(
        level_index,
        [partial(deep_block, branch_level) for branch_level in range(4)],
        tiles,
        kernels,
        biases,
    )
    return tuple(joined(strips, join_weight, join_bias))


def solution(mesh):
    in_specs = (
        P("branch", "row", "col", None, None),
        P("branch", None, None, None, None, None),
        P("branch", None, None),
        P(),
        P(),
    )
    out_specs = (
        P(None, ("branch", "row"), "col"),
        P(None, ("branch", "row"), "col"),
        P(None, ("branch", "row"), "col"),
        P(None, ("branch", "row"), "col"),
    )
    return jax.shard_map(local, mesh=mesh, in_specs=in_specs, out_specs=out_specs, check_vma=False)
```
